32 devices in a mesh: frame: 4 (over z), row: 8 (over y, x, core).
Axes of the slice: x: 2, y: 2, z: 4, core: 2. Of those that a mesh axis runs over, the one named last changes fastest.
Arguments:
- fine: bfloat16 [8, 320, 32, 128], P('frame', None, 'row'), may hold values from -6 to 6
- coarse: bfloat16 [4, 64, 1280], P(None, 'row', 'frame'), may hold values from -6 to 6
- w_qkv: bfloat16 [3, 1280, 1280], P(None, None, 'frame'), may hold values from -0.15625 to 0.15625
- w_out: bfloat16 [1280, 1280], P('frame'), may hold values from -0.15625 to 0.15625
- w_up: bfloat16 [1280, 320], P('frame'), may hold values from -0.15625 to 0.15625
- gain_one: float32 [320], replicated, may hold values from 0.1 to 1.9
- conv_space: bfloat16 [3, 3, 320, 320], replicated, may hold values from -0.109375 to 0.109375
- gain_two: float32 [320], replicated, may hold values from 0.1 to 1.9
- conv_time: bfloat16 [3, 320, 320], replicated, may hold values from -0.1875 to 0.1875
Outputs:
- result: bfloat16 [8, 320, 32, 128], P('frame', None, 'row')
The draws below stay inside these ranges and needn't reach their ends.
All inputs are finite; a program needn't handle non-finite values.
Results may differ from the reference program's by a relative error of at most 0.013.
Values may be sent and summed in bfloat16 or wider, within the bound.
A program may use at most 64 MiB of HBM per device.

```python
import math
import jax
import jax.numpy as jnp
from jax import lax

C = 320
CC = 1280
HEADS = 16
HD = 80
W = 128
CF = 4
FRAMES = 8
ROWS = 32
CH = 4
CW = 16
CP = 64


def shard_levels(own_key, dims, shards, least, top_value):
    def one(dim, parts):
        draws = jax.random.uniform(jax.random.fold_in(jax.random.fold_in(own_key, 6), dim), (parts,), jnp.float32, least / len(shards), top_value / len(shards))
        return jnp.repeat(jnp.exp(draws), dims[dim] // parts).reshape((-1,) + (1,) * (len(dims) - dim - 1))

    loudness = one(*shards[0])
    for cut in shards[1:]:
        loudness = loudness * one(*cut)
    return loudness


def gaussian(rng, shape, scale, most, split=(), held_as=jnp.bfloat16):
    result = scale * jax.random.normal(rng, shape, jnp.float32)
    if split:
        result = result * shard_levels(rng, shape, split, -0.22, 0.18)
    return jnp.clip(result, -most, most).astype(held_as)


def setup_inputs(seed: int = 0) -> dict:
    seeds = jax.random.split(jax.random.key(seed), 10)
    return {
        "fine": gaussian(seeds[0], (FRAMES, C, ROWS, W), 1.0, 6.0, ((0, 4), (2, 8))),
        "coarse": gaussian(seeds[1], (CF, CP, CC), 1.0, 6.0, ((1, 8), (2, 4))),
        "w_qkv": gaussian(seeds[2], (3, CC, CC), CC ** -0.5, 0.15625, ((2, 4),)),
        "w_out": gaussian(seeds[3], (CC, CC), CC ** -0.5, 0.15625, ((0, 4),)),
        "w_up": gaussian(seeds[4], (CC, C), CC ** -0.5, 0.15625, ((0, 4),)),
        "gain_one": jnp.clip(1.0 + 0.18 * jax.random.normal(seeds[5], (C,), jnp.float32), 0.1, 1.9),
        "conv_space": gaussian(seeds[6], (3, 3, C, C), (9 * C) ** -0.5, 0.109375),
        "gain_two": jnp.clip(1.0 + 0.18 * jax.random.normal(seeds[7], (C,), jnp.float32), 0.1, 1.9),
        "conv_time": gaussian(seeds[8], (3, C, C), (3 * C) ** -0.5, 0.1875),
    }


def norm_silu(values, gain):
    square = lax.optimization_barrier(jnp.mean(values * values, axis=-3, keepdims=True))
    scaled = values * lax.rsqrt(square + 1e-06) * gain[:, None, None]
    return jax.nn.silu(scaled).astype(jnp.bfloat16)

def reference(fine, coarse, w_qkv, w_out, w_up, gain_one, conv_space, gain_two, conv_time):
    qkv = jnp.einsum('fpc,icd->ifpd', coarse.astype(jnp.float32), w_qkv.astype(jnp.float32)).astype(jnp.bfloat16)
    query = qkv[0].reshape(CF, CP, HEADS, HD).astype(jnp.float32)
    keys = qkv[1].reshape(CF, CP, HEADS, HD).astype(jnp.float32)
    values = qkv[2].reshape(CF, CP, HEADS, HD).astype(jnp.float32)
    scores = jnp.einsum('fphd,gphd->phfg', query, keys) / math.sqrt(HD)
    probs = jax.nn.softmax(scores, axis=-1).astype(jnp.bfloat16)
    attn = jnp.einsum('phfg,gphd->fphd', probs.astype(jnp.float32), values).astype(jnp.bfloat16).reshape(CF * CP, CC)
    projected = jnp.dot(attn, w_out, preferred_element_type=jnp.float32)
    coarse_out = (coarse.reshape(CF * CP, CC).astype(jnp.float32) + projected).astype(jnp.bfloat16)
    upward = jnp.dot(coarse_out, w_up, preferred_element_type=jnp.float32).astype(jnp.bfloat16)
    upward = upward.reshape(CF, CH, CW, C)

    def first_half(index):
        coarse_frame = (index * CF // FRAMES).astype(jnp.int32)
        cells = lax.dynamic_index_in_dim(upward, coarse_frame, 0, keepdims=False)
        spread = jnp.repeat(jnp.repeat(cells, 8, axis=0), 8, axis=1)
        spread = jnp.transpose(spread, (2, 0, 1)).astype(jnp.float32)
        frame_in = lax.dynamic_index_in_dim(fine, index, 0, keepdims=False).astype(jnp.float32)
        merged = (frame_in + spread).astype(jnp.bfloat16)
        first = norm_silu(merged.astype(jnp.float32), gain_one)
        padded = jnp.pad(first.astype(jnp.float32), ((0, 0), (1, 1), (1, 1)))
        spatial = jnp.zeros((C, ROWS, W), jnp.float32)
        for offset_y in range(3):
            for offset_x in range(3):
                window = padded[:, offset_y:offset_y + ROWS, offset_x:offset_x + W]
                spatial = spatial + jnp.einsum('crw,cd->drw', window, conv_space[offset_y, offset_x].astype(jnp.float32))
        return (merged, norm_silu(spatial, gain_two))
    merged_all, second_all = lax.map(first_half, jnp.arange(FRAMES, dtype=jnp.int32))
    padded_time = jnp.pad(second_all, ((1, 1), (0, 0), (0, 0), (0, 0)))

    def second_half(index):
        window = lax.dynamic_slice_in_dim(padded_time, index, 3, 0)
        temporal = jnp.zeros((C, ROWS, W), jnp.float32)
        for offset in range(3):
            temporal = temporal + jnp.einsum('crw,cd->drw', window[offset].astype(jnp.float32), conv_time[offset].astype(jnp.float32))
        merged = lax.dynamic_index_in_dim(merged_all, index, 0, keepdims=False).astype(jnp.float32)
        return (merged + temporal).astype(jnp.bfloat16)
    return lax.map(second_half, jnp.arange(FRAMES, dtype=jnp.int32))
```

```python
import functools
import math

import jax
import jax.numpy as jnp
from jax import lax
from jax.experimental import pallas as pl
from jax.experimental.pallas import tpu as pltpu
from jax.sharding import PartitionSpec as P

HD = 80
UPSAMPLE = 8
MESH = pl.DeviceIdType.MESH
BF = jnp.bfloat16
F32 = jnp.float32


def silu(a):
    half = 0.5 * a
    return half + half * jnp.tanh(half)


def dot(a, b):
    return jnp.dot(a, b, preferred_element_type=F32)


def dot_t(a, b):
    return lax.dot_general(a, b, (((0,), (0,)), ((), ())), preferred_element_type=F32)


def kernel(
    nf, nr, cf_count, p_dev,
    fine_ref, coarse_ref, w_qkv_ref, w_out_ref, w_up_ref, gain_one_ref, conv_s_ref, gain_two_ref, conv_t_ref,
    out_ref,
    wq, wo, wu, cs, ct, cst, ctt, fb, cg, rs_send, rs_recv, up_send, up_recv, ub_send, ub, x3, n2,
    load_sem, halo_send, halo_recv, g_send, g_recv, r_send, r_recv, u_send, u_recv, b_send, b_recv,
):
    f_dev, rows, chans, width = fine_ref.shape
    cells, c_dev = coarse_ref.shape
    frames_ext = f_dev + 2
    rows_ext = rows + 2
    group = (width // UPSAMPLE) // p_dev
    n_groups = nr // group
    heads = c_dev // HD
    me_f = lax.axis_index("frame")
    me_r = lax.axis_index("row")
    my_group = me_r // group
    k_me = me_r % group
    first = k_me == 0
    last = k_me == group - 1

    loads = [
        pltpu.make_async_copy(src, dst, load_sem.at[n])
        for n, (src, dst) in enumerate(
            (
                (w_qkv_ref, wq),
                (w_out_ref, wo),
                (w_up_ref, wu),
                (conv_s_ref, cs),
                (conv_t_ref, ct),
                (fine_ref, fb.at[pl.ds(1, f_dev), pl.ds(1, rows)]),
            )
        )
    ]
    for load in loads:
        load.start()

    def dev(f, r):
        return {"frame": f, "row": r}

    barrier = pltpu.get_barrier_semaphore()
    expected = jnp.int32(nf - 1)
    for step in range(1, nf):
        pl.semaphore_signal(barrier, inc=1, device_id=dev((me_f + step) % nf, me_r), device_id_type=MESH)
    row_start = my_group * group - group
    for step in range(3 * group):
        peer = row_start + step
        ok = (peer >= 0) & (peer < nr) & (peer != me_r)
        expected = expected + ok.astype(jnp.int32)

        @pl.when(ok)
        def _(peer=peer):
            pl.semaphore_signal(barrier, inc=1, device_id=dev(me_f, peer), device_id_type=MESH)

    for df in (-1, 1):
        for dr in (-1, 1):
            f, r = me_f + df, me_r + dr
            ok = (f >= 0) & (f < nf) & (r >= 0) & (r < nr)
            expected = expected + ok.astype(jnp.int32)

            @pl.when(ok)
            def _(f=f, r=r):
                pl.semaphore_signal(barrier, inc=1, device_id=dev(f, r), device_id_type=MESH)

    cg[me_f] = coarse_ref[...]
    pl.semaphore_wait(barrier, expected)

    def gather_copy(step):
        return pltpu.make_async_remote_copy(
            src_ref=coarse_ref,
            dst_ref=cg.at[me_f],
            send_sem=g_send.at[step - 1],
            recv_sem=g_recv.at[step - 1],
            device_id=dev((me_f + step) % nf, me_r),
            device_id_type=MESH,
        )

    for step in range(1, nf):
        gather_copy(step).start()

    def halo(n, df, dr):
        src_f = pl.ds(0, f_dev) if df == 0 else pl.ds(f_dev - 1 if df > 0 else 0, 1)
        dst_f = pl.ds(1, f_dev) if df == 0 else pl.ds(0 if df > 0 else frames_ext - 1, 1)
        src_r = pl.ds(0, rows) if dr == 0 else pl.ds(rows - 1 if dr > 0 else 0, 1)
        dst_r = pl.ds(1, rows) if dr == 0 else pl.ds(0 if dr > 0 else rows_ext - 1, 1)
        copy = pltpu.make_async_remote_copy(
            src_ref=fine_ref.at[src_f, src_r],
            dst_ref=fb.at[dst_f, dst_r],
            send_sem=halo_send.at[n],
            recv_sem=halo_recv.at[n],
            device_id=dev(me_f + df, me_r + dr),
            device_id_type=MESH,
        )
        there = (me_f + df >= 0) & (me_f + df < nf) & (me_r + dr >= 0) & (me_r + dr < nr)
        source = (me_f - df >= 0) & (me_f - df < nf) & (me_r - dr >= 0) & (me_r - dr < nr)
        return copy, there, source, (dst_f, dst_r)

    offsets = [(df, dr) for df in (-1, 1, 0) for dr in (0, -1, 1) if (df, dr) != (0, 0)]
    for n, (df, dr) in enumerate(offsets):
        copy, there, source, (dst_f, dst_r) = halo(n, df, dr)

        @pl.when(there)
        def _(copy=copy):
            copy.start()

        @pl.when(jnp.logical_not(source))
        def _(dst_f=dst_f, dst_r=dst_r):
            fb[dst_f, dst_r] = jnp.zeros((dst_f.size, dst_r.size, chans, width), BF)

    @pl.when(me_r == 0)
    def _():
        ub[1] = jnp.zeros(ub.shape[1:], BF)

    @pl.when(me_r == nr - 1)
    def _():
        ub[2] = jnp.zeros(ub.shape[1:], BF)

    loads[3].wait()
    loads[4].wait()
    for dy in range(3):
        cst[dy] = cs[dy].T
    ctt[...] = ct[...].T

    loads[0].wait()
    for step in range(1, nf):
        gather_copy(step).wait()
    qkv = []
    for i in range(3):
        total = None
        for j in range(nf):
            term = dot(cg[j], wq[i, j * c_dev : (j + 1) * c_dev, :])
            total = term if total is None else total + term
        qkv.append(total.astype(BF))
    query, keys, values = qkv

    head_of_lane = lax.broadcasted_iota(jnp.int32, (cells, c_dev), 1) // HD
    spread = jnp.concatenate(
        [jnp.where(head_of_lane == h, query.astype(F32), 0.0) for h in range(heads)], axis=0
    ).astype(BF)
    scores = lax.dot_general(
        spread, keys, (((1,), (1,)), ((), ())), preferred_element_type=F32
    ) / math.sqrt(HD)
    cell_q = lax.broadcasted_iota(jnp.int32, scores.shape, 0) % p_dev
    cell_k = lax.broadcasted_iota(jnp.int32, scores.shape, 1) % p_dev
    same = cell_q == cell_k
    scores = jnp.where(same, scores, -1e30)
    top = jnp.max(scores, axis=1, keepdims=True)
    weight = jnp.where(same, jnp.exp(scores - top), 0.0)
    probs = (weight / jnp.sum(weight, axis=1, keepdims=True)).astype(BF)
    mixed = dot(probs, values)
    attn = None
    for h in range(heads):
        part = jnp.where(head_of_lane == h, mixed[h * cells : (h + 1) * cells], 0.0)
        attn = part if attn is None else attn + part
    attn = attn.astype(BF)

    loads[1].wait()
    partial_out = dot(attn, wo[...])
    for j in range(nf):
        rs_send[j] = partial_out[:, j * c_dev : (j + 1) * c_dev].astype(BF)

    def scatter_copy(step):
        peer = (me_f + step) % nf
        return pltpu.make_async_remote_copy(
            src_ref=rs_send.at[peer],
            dst_ref=rs_recv.at[me_f],
            send_sem=r_send.at[step - 1],
            recv_sem=r_recv.at[step - 1],
            device_id=dev(peer, me_r),
            device_id_type=MESH,
        )

    for step in range(1, nf):
        scatter_copy(step).start()
    rs_recv[me_f] = rs_send[me_f]
    loads[2].wait()
    for step in range(1, nf):
        scatter_copy(step).wait()
    share = coarse_ref[...].astype(F32)
    for j in range(nf):
        share = share + rs_recv[j].astype(F32)
    up_partial = dot(share.astype(BF), wu[...]).astype(BF)

    up_send[...] = up_partial
    up_recv[me_f] = up_partial

    def sum_copy(step):
        return pltpu.make_async_remote_copy(
            src_ref=up_send,
            dst_ref=up_recv.at[me_f],
            send_sem=u_send.at[step - 1],
            recv_sem=u_recv.at[step - 1],
            device_id=dev((me_f + step) % nf, me_r),
            device_id_type=MESH,
        )

    for step in range(1, nf):
        sum_copy(step).start()
    for step in range(1, nf):
        sum_copy(step).wait()
    up = up_recv[0].astype(F32)
    for j in range(1, nf):
        up = up + up_recv[j].astype(F32)
    up = up.astype(BF)

    ub_send[...] = up
    ub[0, k_me] = up

    def row_copy(n, region, peer):
        return pltpu.make_async_remote_copy(
            src_ref=ub_send,
            dst_ref=ub.at[region, k_me],
            send_sem=b_send.at[n],
            recv_sem=b_recv.at[region, k_me],
            device_id=dev(me_f, peer),
            device_id_type=MESH,
        )

    def row_arrival(region, k):
        return pltpu.make_async_remote_copy(
            src_ref=ub_send,
            dst_ref=ub.at[region, k],
            send_sem=b_send.at[0],
            recv_sem=b_recv.at[region, k],
            device_id=dev(me_f, me_r),
            device_id_type=MESH,
        )

    base = my_group * group
    targets = [(step - 1, 0, base + (k_me + step) % group, None) for step in range(1, group)]
    targets.append((group - 1, 1, base + group, my_group < n_groups - 1))
    targets.append((group, 2, base - 1, my_group > 0))
    for n, region, peer, ok in targets:
        if ok is None:
            row_copy(n, region, peer).start()
        else:

            @pl.when(ok)
            def _(n=n, region=region, peer=peer):
                row_copy(n, region, peer).start()

    for step in range(1, group):
        row_arrival(0, (k_me + step) % group).wait_recv()

    @pl.when(first & (my_group > 0))
    def _():
        for k in range(group):
            row_arrival(1, k).wait_recv()

    @pl.when(last & (my_group < n_groups - 1))
    def _():
        for k in range(group):
            row_arrival(2, k).wait_recv()

    loads[5].wait()
    for n, (df, dr) in enumerate(offsets):
        copy, there, source, _ = halo(n, df, dr)

        @pl.when(there)
        def _(copy=copy):
            copy.wait_send()

        @pl.when(source)
        def _(copy=copy):
            copy.wait_recv()

    span = group * cells
    lanes = frames_ext * width
    rho = lax.broadcasted_iota(jnp.int32, (span, lanes), 0)
    lane = lax.broadcasted_iota(jnp.int32, (span, lanes), 1)
    total_frames = nf * f_dev
    frame_at = me_f * f_dev - 1 + lane // width
    wanted_frame = (frame_at * cf_count + total_frames) // total_frames - 1
    wanted_cell = (lane % width) // UPSAMPLE
    frame_of = (rho % cells) // p_dev
    cell_of = (rho // cells) * p_dev + rho % p_dev
    pick = jnp.where((wanted_frame == frame_of) & (wanted_cell == cell_of), 1.0, 0.0).astype(BF)

    def widened(region):
        block = [ub[region, k] for k in range(group)]
        block = jnp.concatenate(block, axis=0) if group > 1 else block[0]
        return dot_t(block, pick)

    own = widened(0)
    above = widened(jnp.where(first, 1, 0))
    below = widened(jnp.where(last, 2, 0))
    gain_one = gain_one_ref[...]
    gain_two = gain_two_ref[...]
    column = lax.broadcasted_iota(jnp.int32, (chans, width), 1)
    for t in range(frames_ext):
        window = slice(t * width, (t + 1) * width)
        for r in range(rows_ext):
            spread_up = above if r == 0 else below if r == rows_ext - 1 else own
            merged = (fb[t, r].astype(F32) + spread_up[:, window]).astype(BF)
            if 0 < t < frames_ext - 1 and 0 < r < rows_ext - 1:
                fb[t, r] = merged
            v = merged.astype(F32)
            scale = lax.rsqrt(jnp.mean(v * v, axis=0, keepdims=True) + 1e-06)
            act = silu(v * scale * gain_one)
            here = slice(r * width, (r + 1) * width)
            x3[t % 2, chans : 2 * chans, here] = act.astype(BF)
            left = jnp.where(column == 0, 0.0, pltpu.roll(act, 1, 1))
            right = jnp.where(column == width - 1, 0.0, pltpu.roll(act, width - 1, 1))
            x3[t % 2, 0:chans, here] = left.astype(BF)
            x3[t % 2, 2 * chans : 3 * chans, here] = right.astype(BF)
        spatial = None
        for dy in range(3):
            term = dot(cst[dy], x3[t % 2, :, dy * width : (dy + rows) * width])
            spatial = term if spatial is None else spatial + term
        for r in range(rows):
            here = slice(r * width, (r + 1) * width)
            v = spatial[:, here]
            scale = lax.rsqrt(jnp.mean(v * v, axis=0, keepdims=True) + 1e-06)
            n2[t * chans : (t + 1) * chans, here] = silu(v * scale * gain_two).astype(BF)
    for t in range(f_dev):
        temporal = dot(ctt[...], n2[t * chans : (t + 3) * chans, :])
        for r in range(rows):
            here = slice(r * width, (r + 1) * width)
            out_ref[t, r] = (fb[t + 1, r + 1].astype(F32) + temporal[:, here]).astype(BF)

    for n, region, peer, ok in targets:
        if ok is None:
            row_copy(n, region, peer).wait_send()
        else:

            @pl.when(ok)
            def _(n=n, region=region, peer=peer):
                row_copy(n, region, peer).wait_send()


def local(fine, coarse, w_qkv, w_out, w_up, gain_one, conv_space, gain_two, conv_time):
    nf = lax.axis_size("frame")
    nr = lax.axis_size("row")
    f_dev, chans, rows, width = fine.shape
    cf_count, p_dev, c_dev = coarse.shape
    cells = cf_count * p_dev
    cc = nf * c_dev
    group = (width // UPSAMPLE) // p_dev
    fine_t = jnp.transpose(fine, (0, 2, 1, 3))
    any_spec = pl.BlockSpec(memory_space=pl.ANY)
    vmem = pl.BlockSpec(memory_space=pltpu.VMEM)
    dma = pltpu.SemaphoreType.DMA
    out = pl.pallas_call(
        functools.partial(kernel, nf, nr, cf_count, p_dev),
        out_shape=jax.ShapeDtypeStruct((f_dev, rows, chans, width), BF),
        in_specs=[any_spec, vmem, any_spec, any_spec, any_spec, vmem, any_spec, vmem, any_spec],
        out_specs=vmem,
        scratch_shapes=[
            pltpu.VMEM((3, cc, c_dev), BF),
            pltpu.VMEM((c_dev, cc), BF),
            pltpu.VMEM((c_dev, chans), BF),
            pltpu.VMEM((3, 3 * chans, chans), BF),
            pltpu.VMEM((3 * chans, chans), BF),
            pltpu.VMEM((3, chans, 3 * chans), BF),
            pltpu.VMEM((chans, 3 * chans), BF),
            pltpu.VMEM((f_dev + 2, rows + 2, chans, width), BF),
            pltpu.VMEM((nf, cells, c_dev), BF),
            pltpu.VMEM((nf, cells, c_dev), BF),
            pltpu.VMEM((nf, cells, c_dev), BF),
            pltpu.VMEM((cells, chans), BF),
            pltpu.VMEM((nf, cells, chans), BF),
            pltpu.VMEM((cells, chans), BF),
            pltpu.VMEM((3, group, cells, chans), BF),
            pltpu.VMEM((2, 3 * chans, (rows + 2) * width), BF),
            pltpu.VMEM(((f_dev + 2) * chans, rows * width), BF),
            dma((6,)),
            dma((8,)),
            dma((8,)),
            dma((nf,)),
            dma((nf,)),
            dma((nf,)),
            dma((nf,)),
            dma((nf,)),
            dma((nf,)),
            dma((group + 1,)),
            dma((3, group)),
        ],
        compiler_params=pltpu.CompilerParams(
            collective_id=0, has_side_effects=True, vmem_limit_bytes=56 * 1024 * 1024
        ),
        name="decoder_window",
    )(
        fine_t,
        coarse.reshape(cells, c_dev),
        w_qkv,
        w_out,
        w_up,
        jnp.broadcast_to(gain_one[:, None], (chans, width)),
        conv_space.reshape(3, 3 * chans, chans),
        jnp.broadcast_to(gain_two[:, None], (chans, width)),
        conv_time.reshape(3 * chans, chans),
    )
    return jnp.transpose(out, (0, 2, 1, 3))


def solution(mesh):
    return jax.shard_map(
        local,
        mesh=mesh,
        in_specs=(
            P("frame", None, "row", None),
            P(None, "row", "frame"),
            P(None, None, "frame"),
            P("frame", None),
            P("frame", None),
            P(),
            P(),
            P(),
            P(),
        ),
        out_specs=P("frame", None, "row", None),
        check_vma=False,
    )
```

```python
import functools
import math

import jax
import jax.numpy as jnp
from jax import lax
from jax.experimental import pallas as pl
from jax.experimental.pallas import tpu as pltpu
from jax.sharding import PartitionSpec as P

HD = 80
UPSAMPLE = 8
MESH = pl.DeviceIdType.MESH
BF = jnp.bfloat16
F32 = jnp.float32


def silu(a):
    half = 0.5 * a
    return half + half * jnp.tanh(half)


def dot(a, b):
    return jnp.dot(a, b, preferred_element_type=F32)


def dot_t(a, b):
    return lax.dot_general(a, b, (((0,), (0,)), ((), ())), preferred_element_type=F32)


def kernel(
    nf, nr, cf_count, p_dev,
    fine_ref, coarse_ref, w_qkv_ref, w_out_ref, w_up_ref, gain_one_ref, conv_s_ref, gain_two_ref, conv_t_ref,
    out_ref,
    wq, wo, wu, cs, ct, cst, ctt, fb, cg, rs_send, rs_recv, up_send, up_recv, ub_send, ub, x3, n2, gain_one, gain_two,
    load_sem, halo_send, halo_recv, g_send, g_recv, r_send, r_recv, u_send, u_recv, b_send, b_recv,
):
    f_dev, rows, chans, width = fine_ref.shape
    cells, c_dev = coarse_ref.shape
    frames_ext = f_dev + 2
    rows_ext = rows + 2
    group = (width // UPSAMPLE) // p_dev
    n_groups = nr // group
    heads = c_dev // HD
    me_f = lax.axis_index("frame")
    me_r = lax.axis_index("row")
    my_group = me_r // group
    k_me = me_r % group
    first = k_me == 0
    last = k_me == group - 1

    parts = {
        "space0": (conv_s_ref.at[0], cs.at[0]),
        "qkv": (w_qkv_ref, wq),
        "out": (w_out_ref, wo),
        "space1": (conv_s_ref.at[1], cs.at[1]),
        "up": (w_up_ref, wu),
        "space2": (conv_s_ref.at[2], cs.at[2]),
        "time": (conv_t_ref, ct),
        "fine": (fine_ref, fb.at[pl.ds(1, f_dev), pl.ds(1, rows)]),
    }
    loads = {
        name: pltpu.make_async_copy(src, dst, load_sem.at[n])
        for n, (name, (src, dst)) in enumerate(parts.items())
    }
    for load in loads.values():
        load.start()

    def dev(f, r):
        return {"frame": f, "row": r}

    barrier = pltpu.get_barrier_semaphore()
    expected = jnp.int32(nf - 1)
    for step in range(1, nf):
        pl.semaphore_signal(barrier, inc=1, device_id=dev((me_f + step) % nf, me_r), device_id_type=MESH)
    row_start = my_group * group - group
    for step in range(3 * group):
        peer = row_start + step
        ok = (peer >= 0) & (peer < nr) & (peer != me_r)
        expected = expected + ok.astype(jnp.int32)

        @pl.when(ok)
        def _(peer=peer):
            pl.semaphore_signal(barrier, inc=1, device_id=dev(me_f, peer), device_id_type=MESH)

    cg[me_f] = coarse_ref[...]
    pl.semaphore_wait(barrier, expected)

    def gather_copy(step):
        return pltpu.make_async_remote_copy(
            src_ref=coarse_ref,
            dst_ref=cg.at[me_f],
            send_sem=g_send.at[step - 1],
            recv_sem=g_recv.at[step - 1],
            device_id=dev((me_f + step) % nf, me_r),
            device_id_type=MESH,
        )

    for step in range(1, nf):
        gather_copy(step).start()

    def remote(n, src, dst, f, r):
        return pltpu.make_async_remote_copy(
            src_ref=src,
            dst_ref=dst,
            send_sem=halo_send.at[n],
            recv_sem=halo_recv.at[n],
            device_id=dev(f, r),
            device_id_type=MESH,
        )

    own_f, own_r = pl.ds(1, f_dev), pl.ds(1, rows)
    cut = (rows + 1) // 2
    pieces = [(0, cut), (cut, rows - cut)]
    row_halo, frame_halo, corner_halo = [], [[], []], []
    for n, d in enumerate((-1, 1)):
        there = (me_r + d >= 0) & (me_r + d < nr)
        source = (me_r - d >= 0) & (me_r - d < nr)
        src_r, dst_r = (rows - 1, 0) if d > 0 else (0, rows_ext - 1)
        row_halo.append(
            (
                remote(n, fine_ref.at[:, pl.ds(src_r, 1)], fb.at[own_f, pl.ds(dst_r, 1)], me_f, me_r + d),
                there,
                source,
            )
        )

        @pl.when(jnp.logical_not(source))
        def _(dst_r=dst_r):
            fb[:, dst_r] = jnp.zeros((frames_ext, chans, width), BF)

        for e, at in enumerate((0, frames_ext - 1)):
            corner_halo.append(
                (
                    remote(6 + 2 * n + e, fb.at[at, src_r + 1], fb.at[at, dst_r], me_f, me_r + d),
                    there & (me_f > 0 if e == 0 else me_f < nf - 1),
                    source & (me_f > 0 if e == 0 else me_f < nf - 1),
                )
            )
        there = (me_f + d >= 0) & (me_f + d < nf)
        source = (me_f - d >= 0) & (me_f - d < nf)
        src_f, dst_f = (f_dev - 1, 0) if d > 0 else (0, frames_ext - 1)
        for piece, (start, size) in enumerate(pieces):
            if size:
                copy = remote(
                    2 + 2 * n + piece,
                    fine_ref.at[src_f, pl.ds(start, size)],
                    fb.at[dst_f, pl.ds(1 + start, size)],
                    me_f + d,
                    me_r,
                )
                frame_halo[piece].append((copy, there, source))

        @pl.when(jnp.logical_not(source))
        def _(dst_f=dst_f):
            fb[dst_f] = jnp.zeros((rows_ext, chans, width), BF)

    def start_all(copies):
        for copy, there, _ in copies:

            @pl.when(there)
            def _(copy=copy):
                copy.start()

    def arrive_all(copies):
        for copy, _, source in copies:

            @pl.when(source)
            def _(copy=copy):
                copy.wait_recv()

    def sent_all(copies):
        for copy, there, _ in copies:

            @pl.when(there)
            def _(copy=copy):
                copy.wait_send()

    start_all(frame_halo[0])
    start_all(row_halo)

    @pl.when(me_r == 0)
    def _():
        ub[1] = jnp.zeros(ub.shape[1:], BF)

    @pl.when(me_r == nr - 1)
    def _():
        ub[2] = jnp.zeros(ub.shape[1:], BF)

    gain_one[...] = jnp.broadcast_to(gain_one_ref[...], (width, chans)).T
    gain_two[...] = jnp.broadcast_to(gain_two_ref[...], (width, chans)).T

    def turn(dy):
        loads[f"space{dy}"].wait()
        cst[dy] = cs[dy].T

    turn(0)
    loads["qkv"].wait()
    for step in range(1, nf):
        gather_copy(step).wait()
    cells_all = jnp.concatenate([cg[j].astype(F32) for j in range(nf)], axis=1).astype(BF)
    qkv = []
    for i in range(3):
        product = lax.dot_general(
            cells_all, wq[i], (((1,), (1,)), ((), ())), preferred_element_type=F32
        )
        qkv.append(product.astype(BF))
    query, keys, values = qkv

    head_of_lane = lax.broadcasted_iota(jnp.int32, (cells, c_dev), 1) // HD
    spread = jnp.concatenate(
        [jnp.where(head_of_lane == h, query.astype(F32), 0.0) for h in range(heads)], axis=0
    ).astype(BF)
    scores = lax.dot_general(
        spread, keys, (((1,), (1,)), ((), ())), preferred_element_type=F32
    ) / math.sqrt(HD)
    cell_q = lax.broadcasted_iota(jnp.int32, scores.shape, 0) % p_dev
    cell_k = lax.broadcasted_iota(jnp.int32, scores.shape, 1) % p_dev
    same = cell_q == cell_k
    scores = jnp.where(same, scores, -1e30)
    top = jnp.max(scores, axis=1, keepdims=True)
    weight = jnp.where(same, jnp.exp(scores - top), 0.0)
    probs = (weight / jnp.sum(weight, axis=1, keepdims=True)).astype(BF)
    mixed = dot(probs, values)
    attn = None
    for h in range(heads):
        part = jnp.where(head_of_lane == h, mixed[h * cells : (h + 1) * cells], 0.0)
        attn = part if attn is None else attn + part
    attn = attn.astype(BF)

    loads["out"].wait()
    partial_out = dot(attn, wo[...])
    for j in range(nf):
        rs_send[j] = partial_out[:, j * c_dev : (j + 1) * c_dev].astype(BF)

    def scatter_copy(step):
        peer = (me_f + step) % nf
        return pltpu.make_async_remote_copy(
            src_ref=rs_send.at[peer],
            dst_ref=rs_recv.at[me_f],
            send_sem=r_send.at[step - 1],
            recv_sem=r_recv.at[step - 1],
            device_id=dev(peer, me_r),
            device_id_type=MESH,
        )

    for step in range(1, nf):
        scatter_copy(step).start()
    rs_recv[me_f] = rs_send[me_f]
    turn(1)
    loads["up"].wait()
    for step in range(1, nf):
        scatter_copy(step).wait()
    share = coarse_ref[...].astype(F32)
    for j in range(nf):
        share = share + rs_recv[j].astype(F32)
    up_partial = dot(share.astype(BF), wu[...]).astype(BF)

    up_send[...] = up_partial
    up_recv[me_f] = up_partial

    def sum_copy(step):
        return pltpu.make_async_remote_copy(
            src_ref=up_send,
            dst_ref=up_recv.at[me_f],
            send_sem=u_send.at[step - 1],
            recv_sem=u_recv.at[step - 1],
            device_id=dev((me_f + step) % nf, me_r),
            device_id_type=MESH,
        )

    for step in range(1, nf):
        sum_copy(step).start()
    start_all(frame_halo[1])
    turn(2)
    for step in range(1, nf):
        sum_copy(step).wait()
    up = up_recv[0].astype(F32)
    for j in range(1, nf):
        up = up + up_recv[j].astype(F32)
    up = up.astype(BF)

    ub_send[...] = up
    ub[0, k_me] = up

    def row_copy(n, region, peer):
        return pltpu.make_async_remote_copy(
            src_ref=ub_send,
            dst_ref=ub.at[region, k_me],
            send_sem=b_send.at[n],
            recv_sem=b_recv.at[region, k_me],
            device_id=dev(me_f, peer),
            device_id_type=MESH,
        )

    def row_arrival(region, k):
        return pltpu.make_async_remote_copy(
            src_ref=ub_send,
            dst_ref=ub.at[region, k],
            send_sem=b_send.at[0],
            recv_sem=b_recv.at[region, k],
            device_id=dev(me_f, me_r),
            device_id_type=MESH,
        )

    base = my_group * group
    targets = [(step - 1, 0, base + (k_me + step) % group, None) for step in range(1, group)]
    targets.append((group - 1, 1, base + group, my_group < n_groups - 1))
    targets.append((group, 2, base - 1, my_group > 0))
    for n, region, peer, ok in targets:
        if ok is None:
            row_copy(n, region, peer).start()
        else:

            @pl.when(ok)
            def _(n=n, region=region, peer=peer):
                row_copy(n, region, peer).start()

    loads["time"].wait()
    ctt[...] = ct[...].T
    span = group * cells
    lanes = frames_ext * width
    rho = lax.broadcasted_iota(jnp.int32, (span, lanes), 0)
    lane = lax.broadcasted_iota(jnp.int32, (span, lanes), 1)
    total_frames = nf * f_dev
    frame_at = me_f * f_dev - 1 + lane // width
    wanted_frame = (frame_at * cf_count + total_frames) // total_frames - 1
    wanted_cell = (lane % width) // UPSAMPLE
    frame_of = (rho % cells) // p_dev
    cell_of = (rho // cells) * p_dev + rho % p_dev
    pick = jnp.where((wanted_frame == frame_of) & (wanted_cell == cell_of), 1.0, 0.0).astype(BF)

    loads["fine"].wait()
    arrive_all(row_halo)
    for step in range(1, group):
        row_arrival(0, (k_me + step) % group).wait_recv()

    @pl.when(first & (my_group > 0))
    def _():
        for k in range(group):
            row_arrival(1, k).wait_recv()

    @pl.when(last & (my_group < n_groups - 1))
    def _():
        for k in range(group):
            row_arrival(2, k).wait_recv()

    def widened(region):
        block = [ub[region, k] for k in range(group)]
        block = jnp.concatenate(block, axis=0) if group > 1 else block[0]
        return dot_t(block, pick)

    own = widened(0)
    above = widened(jnp.where(first, 1, 0))
    below = widened(jnp.where(last, 2, 0))
    column = lax.broadcasted_iota(jnp.int32, (chans, width), 1)
    for place, t in enumerate([*range(1, frames_ext - 1), 0, frames_ext - 1]):
        if place == 1:
            arrive_all(frame_halo[0])
            arrive_all(frame_halo[1])
            start_all(corner_halo)
        if t == 0:
            arrive_all(corner_halo)
        slot = place % 2
        window = slice(t * width, (t + 1) * width)
        for r in range(rows_ext):
            spread_up = above if r == 0 else below if r == rows_ext - 1 else own
            merged = (fb[t, r].astype(F32) + spread_up[:, window]).astype(BF)
            if 0 < t < frames_ext - 1 and 0 < r < rows_ext - 1:
                fb[t, r] = merged
            v = merged.astype(F32)
            scale = lax.rsqrt(jnp.mean(v * v, axis=0, keepdims=True) + 1e-06)
            act = silu(v * scale * gain_one[...])
            here = slice(r * width, (r + 1) * width)
            x3[slot, chans : 2 * chans, here] = act.astype(BF)
            left = jnp.where(column == 0, 0.0, pltpu.roll(act, 1, 1))
            right = jnp.where(column == width - 1, 0.0, pltpu.roll(act, width - 1, 1))
            x3[slot, 0:chans, here] = left.astype(BF)
            x3[slot, 2 * chans : 3 * chans, here] = right.astype(BF)
        spatial = None
        for dy in range(3):
            term = dot(cst[dy], x3[slot, :, dy * width : (dy + rows) * width])
            spatial = term if spatial is None else spatial + term
        for r in range(rows):
            here = slice(r * width, (r + 1) * width)
            v = spatial[:, here]
            scale = lax.rsqrt(jnp.mean(v * v, axis=0, keepdims=True) + 1e-06)
            n2[t * chans : (t + 1) * chans, here] = silu(v * scale * gain_two[...]).astype(BF)
    for t in range(f_dev):
        temporal = dot(ctt[...], n2[t * chans : (t + 3) * chans, :])
        for r in range(rows):
            here = slice(r * width, (r + 1) * width)
            out_ref[t, r] = (fb[t + 1, r + 1].astype(F32) + temporal[:, here]).astype(BF)

    sent_all([*row_halo, *frame_halo[0], *frame_halo[1], *corner_halo])
    for n, region, peer, ok in targets:
        if ok is None:
            row_copy(n, region, peer).wait_send()
        else:

            @pl.when(ok)
            def _(n=n, region=region, peer=peer):
                row_copy(n, region, peer).wait_send()


def local(fine, coarse, w_qkv, w_out, w_up, gain_one, conv_space, gain_two, conv_time):
    nf = lax.axis_size("frame")
    nr = lax.axis_size("row")
    f_dev, chans, rows, width = fine.shape
    cf_count, p_dev, c_dev = coarse.shape
    cells = cf_count * p_dev
    cc = nf * c_dev
    group = (width // UPSAMPLE) // p_dev
    fine_t = jnp.transpose(fine, (0, 2, 1, 3))
    any_spec = pl.BlockSpec(memory_space=pl.ANY)
    vmem = pl.BlockSpec(memory_space=pltpu.VMEM)
    dma = pltpu.SemaphoreType.DMA
    out = pl.pallas_call(
        functools.partial(kernel, nf, nr, cf_count, p_dev),
        out_shape=jax.ShapeDtypeStruct((f_dev, rows, chans, width), BF),
        in_specs=[any_spec, vmem, any_spec, any_spec, any_spec, vmem, any_spec, vmem, any_spec],
        out_specs=vmem,
        scratch_shapes=[
            pltpu.VMEM((3, c_dev, cc), BF),
            pltpu.VMEM((c_dev, cc), BF),
            pltpu.VMEM((c_dev, chans), BF),
            pltpu.VMEM((3, 3 * chans, chans), BF),
            pltpu.VMEM((3 * chans, chans), BF),
            pltpu.VMEM((3, chans, 3 * chans), BF),
            pltpu.VMEM((chans, 3 * chans), BF),
            pltpu.VMEM((f_dev + 2, rows + 2, chans, width), BF),
            pltpu.VMEM((nf, cells, c_dev), BF),
            pltpu.VMEM((nf, cells, c_dev), BF),
            pltpu.VMEM((nf, cells, c_dev), BF),
            pltpu.VMEM((cells, chans), BF),
            pltpu.VMEM((nf, cells, chans), BF),
            pltpu.VMEM((cells, chans), BF),
            pltpu.VMEM((3, group, cells, chans), BF),
            pltpu.VMEM((2, 3 * chans, (rows + 2) * width), BF),
            pltpu.VMEM(((f_dev + 2) * chans, rows * width), BF),
            pltpu.VMEM((chans, width), F32),
            pltpu.VMEM((chans, width), F32),
            dma((8,)),
            dma((10,)),
            dma((10,)),
            dma((nf,)),
            dma((nf,)),
            dma((nf,)),
            dma((nf,)),
            dma((nf,)),
            dma((nf,)),
            dma((group + 1,)),
            dma((3, group)),
        ],
        compiler_params=pltpu.CompilerParams(
            collective_id=0, has_side_effects=True, vmem_limit_bytes=56 * 1024 * 1024
        ),
        name="decoder_window",
    )(
        fine_t,
        coarse.reshape(cells, c_dev),
        jnp.swapaxes(w_qkv, 1, 2),
        w_out,
        w_up,
        gain_one.reshape(1, chans),
        conv_space.reshape(3, 3 * chans, chans),
        gain_two.reshape(1, chans),
        conv_time.reshape(3 * chans, chans),
    )
    return jnp.transpose(out, (0, 2, 1, 3))


def solution(mesh):
    return jax.shard_map(
        local,
        mesh=mesh,
        in_specs=(
            P("frame", None, "row", None),
            P(None, "row", "frame"),
            P(None, None, "frame"),
            P("frame", None),
            P("frame", None),
            P(),
            P(),
            P(),
            P(),
        ),
        out_specs=P("frame", None, "row", None),
        check_vma=False,
    )
```

```python
import functools
import math

import jax
import jax.numpy as jnp
from jax import lax
from jax.experimental import pallas as pl
from jax.experimental.pallas import tpu as pltpu
from jax.sharding import PartitionSpec as P

HD = 80
UPSAMPLE = 8
MESH = pl.DeviceIdType.MESH
BF = jnp.bfloat16
F32 = jnp.float32


def silu(a):
    half = 0.5 * a
    return half + half * jnp.tanh(half)


def dot(a, b):
    return jnp.dot(a, b, preferred_element_type=F32)


def dot_t(a, b):
    return lax.dot_general(a, b, (((0,), (0,)), ((), ())), preferred_element_type=F32)


def kernel(
    nf, nr, cf_count, p_dev,
    fine_ref, coarse_ref, w_qkv_ref, w_out_ref, w_up_ref, gain_one_ref, conv_s_ref, gain_two_ref, conv_t_ref,
    out_ref,
    wq, wo, wu, cs, ct, cst, ctt, fb, cg, rs_send, rs_recv, up_send, up_recv, ub_send, ub, x3, n2, gain_one, gain_two,
    load_sem, halo_send, halo_recv, g_send, g_recv, r_send, r_recv, u_send, u_recv, b_send, b_recv,
):
    f_dev, rows, chans, width = fine_ref.shape
    cells, c_dev = coarse_ref.shape
    frames_ext = f_dev + 2
    rows_ext = rows + 2
    group = (width // UPSAMPLE) // p_dev
    n_groups = nr // group
    heads = c_dev // HD
    me_f = lax.axis_index("frame")
    me_r = lax.axis_index("row")
    my_group = me_r // group
    k_me = me_r % group
    first = k_me == 0
    last = k_me == group - 1

    parts = {
        "space0": (conv_s_ref.at[0], cs.at[0]),
        "qkv": (w_qkv_ref, wq),
        "out": (w_out_ref, wo),
        "space1": (conv_s_ref.at[1], cs.at[1]),
        "up": (w_up_ref, wu),
        "space2": (conv_s_ref.at[2], cs.at[2]),
        "time": (conv_t_ref, ct),
        "fine": (fine_ref, fb.at[pl.ds(1, f_dev), pl.ds(1, rows)]),
    }
    loads = {
        name: pltpu.make_async_copy(src, dst, load_sem.at[n])
        for n, (name, (src, dst)) in enumerate(parts.items())
    }
    for load in loads.values():
        load.start()

    def dev(f, r):
        return {"frame": f, "row": r}

    barrier = pltpu.get_barrier_semaphore()
    expected = jnp.int32(nf - 1)
    for step in range(1, nf):
        pl.semaphore_signal(barrier, inc=1, device_id=dev((me_f + step) % nf, me_r), device_id_type=MESH)
    row_start = my_group * group - group
    for step in range(3 * group):
        peer = row_start + step
        ok = (peer >= 0) & (peer < nr) & (peer != me_r)
        expected = expected + ok.astype(jnp.int32)

        @pl.when(ok)
        def _(peer=peer):
            pl.semaphore_signal(barrier, inc=1, device_id=dev(me_f, peer), device_id_type=MESH)

    cg[me_f] = coarse_ref[...]
    pl.semaphore_wait(barrier, expected)

    def gather_copy(step):
        return pltpu.make_async_remote_copy(
            src_ref=coarse_ref,
            dst_ref=cg.at[me_f],
            send_sem=g_send.at[step - 1],
            recv_sem=g_recv.at[step - 1],
            device_id=dev((me_f + step) % nf, me_r),
            device_id_type=MESH,
        )

    for step in range(1, nf):
        gather_copy(step).start()

    def remote(n, src, dst, f, r):
        return pltpu.make_async_remote_copy(
            src_ref=src,
            dst_ref=dst,
            send_sem=halo_send.at[n],
            recv_sem=halo_recv.at[n],
            device_id=dev(f, r),
            device_id_type=MESH,
        )

    own_f, own_r = pl.ds(1, f_dev), pl.ds(1, rows)
    cut = (rows + 1) // 2
    pieces = [(0, cut), (cut, rows - cut)]
    row_halo, frame_halo, corner_halo = [], [[], []], []
    for n, d in enumerate((-1, 1)):
        there = (me_r + d >= 0) & (me_r + d < nr)
        source = (me_r - d >= 0) & (me_r - d < nr)
        src_r, dst_r = (rows - 1, 0) if d > 0 else (0, rows_ext - 1)
        row_halo.append(
            (
                remote(n, fine_ref.at[:, pl.ds(src_r, 1)], fb.at[own_f, pl.ds(dst_r, 1)], me_f, me_r + d),
                there,
                source,
            )
        )

        @pl.when(jnp.logical_not(source))
        def _(dst_r=dst_r):
            fb[:, dst_r] = jnp.zeros((frames_ext, chans, width), BF)

        for e, at in enumerate((0, frames_ext - 1)):
            corner_halo.append(
                (
                    remote(6 + 2 * n + e, fb.at[at, src_r + 1], fb.at[at, dst_r], me_f, me_r + d),
                    there & (me_f > 0 if e == 0 else me_f < nf - 1),
                    source & (me_f > 0 if e == 0 else me_f < nf - 1),
                )
            )
        there = (me_f + d >= 0) & (me_f + d < nf)
        source = (me_f - d >= 0) & (me_f - d < nf)
        src_f, dst_f = (f_dev - 1, 0) if d > 0 else (0, frames_ext - 1)
        for piece, (start, size) in enumerate(pieces):
            if size:
                copy = remote(
                    2 + 2 * n + piece,
                    fine_ref.at[src_f, pl.ds(start, size)],
                    fb.at[dst_f, pl.ds(1 + start, size)],
                    me_f + d,
                    me_r,
                )
                frame_halo[piece].append((copy, there, source))

        @pl.when(jnp.logical_not(source))
        def _(dst_f=dst_f):
            fb[dst_f] = jnp.zeros((rows_ext, chans, width), BF)

    def start_all(copies):
        for copy, there, _ in copies:

            @pl.when(there)
            def _(copy=copy):
                copy.start()

    def arrive_all(copies):
        for copy, _, source in copies:

            @pl.when(source)
            def _(copy=copy):
                copy.wait_recv()

    def sent_all(copies):
        for copy, there, _ in copies:

            @pl.when(there)
            def _(copy=copy):
                copy.wait_send()

    start_all(frame_halo[0])
    start_all(row_halo)

    @pl.when(me_r == 0)
    def _():
        ub[1] = jnp.zeros(ub.shape[1:], BF)

    @pl.when(me_r == nr - 1)
    def _():
        ub[2] = jnp.zeros(ub.shape[1:], BF)

    gain_one[...] = jnp.broadcast_to(gain_one_ref[...][None, :], (width, chans)).T
    gain_two[...] = jnp.broadcast_to(gain_two_ref[...][None, :], (width, chans)).T

    def turn(dy):
        loads[f"space{dy}"].wait()
        cst[dy] = cs[dy].T

    turn(0)
    loads["qkv"].wait()
    for step in range(1, nf):
        gather_copy(step).wait()
    cells_all = jnp.concatenate([cg[j].astype(F32) for j in range(nf)], axis=1).astype(BF)
    qkv = []
    for i in range(3):
        product = lax.dot_general(
            cells_all, wq[i], (((1,), (1,)), ((), ())), preferred_element_type=F32
        )
        qkv.append(product.astype(BF))
    query, keys, values = qkv

    head_of_lane = lax.broadcasted_iota(jnp.int32, (cells, c_dev), 1) // HD
    spread = jnp.concatenate(
        [jnp.where(head_of_lane == h, query.astype(F32), 0.0) for h in range(heads)], axis=0
    ).astype(BF)
    scores = lax.dot_general(
        spread, keys, (((1,), (1,)), ((), ())), preferred_element_type=F32
    ) / math.sqrt(HD)
    cell_q = lax.broadcasted_iota(jnp.int32, scores.shape, 0) % p_dev
    cell_k = lax.broadcasted_iota(jnp.int32, scores.shape, 1) % p_dev
    same = cell_q == cell_k
    scores = jnp.where(same, scores, -1e30)
    top = jnp.max(scores, axis=1, keepdims=True)
    weight = jnp.where(same, jnp.exp(scores - top), 0.0)
    probs = (weight / jnp.sum(weight, axis=1, keepdims=True)).astype(BF)
    mixed = dot(probs, values)
    attn = None
    for h in range(heads):
        part = jnp.where(head_of_lane == h, mixed[h * cells : (h + 1) * cells], 0.0)
        attn = part if attn is None else attn + part
    attn = attn.astype(BF)

    loads["out"].wait()
    partial_out = dot(attn, wo[...])
    for j in range(nf):
        rs_send[j] = partial_out[:, j * c_dev : (j + 1) * c_dev].astype(BF)

    def scatter_copy(step):
        peer = (me_f + step) % nf
        return pltpu.make_async_remote_copy(
            src_ref=rs_send.at[peer],
            dst_ref=rs_recv.at[me_f],
            send_sem=r_send.at[step - 1],
            recv_sem=r_recv.at[step - 1],
            device_id=dev(peer, me_r),
            device_id_type=MESH,
        )

    for step in range(1, nf):
        scatter_copy(step).start()
    rs_recv[me_f] = rs_send[me_f]
    turn(1)
    loads["up"].wait()
    for step in range(1, nf):
        scatter_copy(step).wait()
    share = coarse_ref[...].astype(F32)
    for j in range(nf):
        share = share + rs_recv[j].astype(F32)
    up_partial = dot(share.astype(BF), wu[...]).astype(BF)

    up_send[...] = up_partial
    up_recv[me_f] = up_partial

    def sum_copy(step):
        return pltpu.make_async_remote_copy(
            src_ref=up_send,
            dst_ref=up_recv.at[me_f],
            send_sem=u_send.at[step - 1],
            recv_sem=u_recv.at[step - 1],
            device_id=dev((me_f + step) % nf, me_r),
            device_id_type=MESH,
        )

    for step in range(1, nf):
        sum_copy(step).start()
    start_all(frame_halo[1])
    turn(2)
    for step in range(1, nf):
        sum_copy(step).wait()
    up = up_recv[0].astype(F32)
    for j in range(1, nf):
        up = up + up_recv[j].astype(F32)
    up = up.astype(BF)

    ub_send[...] = up
    ub[0, k_me] = up

    def row_copy(n, region, peer):
        return pltpu.make_async_remote_copy(
            src_ref=ub_send,
            dst_ref=ub.at[region, k_me],
            send_sem=b_send.at[n],
            recv_sem=b_recv.at[region, k_me],
            device_id=dev(me_f, peer),
            device_id_type=MESH,
        )

    def row_arrival(region, k):
        return pltpu.make_async_remote_copy(
            src_ref=ub_send,
            dst_ref=ub.at[region, k],
            send_sem=b_send.at[0],
            recv_sem=b_recv.at[region, k],
            device_id=dev(me_f, me_r),
            device_id_type=MESH,
        )

    base = my_group * group
    targets = [(step - 1, 0, base + (k_me + step) % group, None) for step in range(1, group)]
    targets.append((group - 1, 1, base + group, my_group < n_groups - 1))
    targets.append((group, 2, base - 1, my_group > 0))
    for n, region, peer, ok in targets:
        if ok is None:
            row_copy(n, region, peer).start()
        else:

            @pl.when(ok)
            def _(n=n, region=region, peer=peer):
                row_copy(n, region, peer).start()

    loads["time"].wait()
    ctt[...] = ct[...].T
    span = group * cells
    lanes = frames_ext * width
    rho = lax.broadcasted_iota(jnp.int32, (span, lanes), 0)
    lane = lax.broadcasted_iota(jnp.int32, (span, lanes), 1)
    total_frames = nf * f_dev
    frame_at = me_f * f_dev - 1 + lane // width
    wanted_frame = (frame_at * cf_count + total_frames) // total_frames - 1
    wanted_cell = (lane % width) // UPSAMPLE
    frame_of = (rho % cells) // p_dev
    cell_of = (rho // cells) * p_dev + rho % p_dev
    pick = jnp.where((wanted_frame == frame_of) & (wanted_cell == cell_of), 1.0, 0.0).astype(BF)

    loads["fine"].wait()
    arrive_all(row_halo)
    for step in range(1, group):
        row_arrival(0, (k_me + step) % group).wait_recv()

    @pl.when(first & (my_group > 0))
    def _():
        for k in range(group):
            row_arrival(1, k).wait_recv()

    @pl.when(last & (my_group < n_groups - 1))
    def _():
        for k in range(group):
            row_arrival(2, k).wait_recv()

    def widened(region):
        block = [ub[region, k] for k in range(group)]
        block = jnp.concatenate(block, axis=0) if group > 1 else block[0]
        return dot_t(block, pick)

    own = widened(0)
    above = widened(jnp.where(first, 1, 0))
    below = widened(jnp.where(last, 2, 0))
    column = lax.broadcasted_iota(jnp.int32, (chans, width), 1)
    for place, t in enumerate([*range(1, frames_ext - 1), 0, frames_ext - 1]):
        if place == 1:
            arrive_all(frame_halo[0])
            arrive_all(frame_halo[1])
            start_all(corner_halo)
        if t == 0:
            arrive_all(corner_halo)
        slot = place % 2
        window = slice(t * width, (t + 1) * width)
        for r in range(rows_ext):
            spread_up = above if r == 0 else below if r == rows_ext - 1 else own
            merged = (fb[t, r].astype(F32) + spread_up[:, window]).astype(BF)
            if 0 < t < frames_ext - 1 and 0 < r < rows_ext - 1:
                fb[t, r] = merged
            v = merged.astype(F32)
            scale = lax.rsqrt(jnp.mean(v * v, axis=0, keepdims=True) + 1e-06)
            act = silu(v * scale * gain_one[...])
            here = slice(r * width, (r + 1) * width)
            x3[slot, chans : 2 * chans, here] = act.astype(BF)
            left = jnp.where(column == 0, 0.0, pltpu.roll(act, 1, 1))
            right = jnp.where(column == width - 1, 0.0, pltpu.roll(act, width - 1, 1))
            x3[slot, 0:chans, here] = left.astype(BF)
            x3[slot, 2 * chans : 3 * chans, here] = right.astype(BF)
        spatial = None
        for dy in range(3):
            term = dot(cst[dy], x3[slot, :, dy * width : (dy + rows) * width])
            spatial = term if spatial is None else spatial + term
        for r in range(rows):
            here = slice(r * width, (r + 1) * width)
            v = spatial[:, here]
            scale = lax.rsqrt(jnp.mean(v * v, axis=0, keepdims=True) + 1e-06)
            n2[t * chans : (t + 1) * chans, here] = silu(v * scale * gain_two[...]).astype(BF)
    for t in range(f_dev):
        temporal = dot(ctt[...], n2[t * chans : (t + 3) * chans, :])
        for r in range(rows):
            here = slice(r * width, (r + 1) * width)
            out_ref[t, r] = (fb[t + 1, r + 1].astype(F32) + temporal[:, here]).astype(BF)

    sent_all([*row_halo, *frame_halo[0], *frame_halo[1], *corner_halo])
    for n, region, peer, ok in targets:
        if ok is None:
            row_copy(n, region, peer).wait_send()
        else:

            @pl.when(ok)
            def _(n=n, region=region, peer=peer):
                row_copy(n, region, peer).wait_send()


def local(fine, coarse, w_qkv, w_out, w_up, gain_one, conv_space, gain_two, conv_time):
    nf = lax.axis_size("frame")
    nr = lax.axis_size("row")
    f_dev, chans, rows, width = fine.shape
    cf_count, p_dev, c_dev = coarse.shape
    cells = cf_count * p_dev
    cc = nf * c_dev
    group = (width // UPSAMPLE) // p_dev
    fine_t = jnp.transpose(fine, (0, 2, 1, 3))
    any_spec = pl.BlockSpec(memory_space=pl.ANY)
    vmem = pl.BlockSpec(memory_space=pltpu.VMEM)
    dma = pltpu.SemaphoreType.DMA
    out = pl.pallas_call(
        functools.partial(kernel, nf, nr, cf_count, p_dev),
        out_shape=jax.ShapeDtypeStruct((f_dev, rows, chans, width), BF),
        in_specs=[any_spec, vmem, any_spec, any_spec, any_spec, vmem, any_spec, vmem, any_spec],
        out_specs=vmem,
        scratch_shapes=[
            pltpu.VMEM((3, c_dev, cc), BF),
            pltpu.VMEM((c_dev, cc), BF),
            pltpu.VMEM((c_dev, chans), BF),
            pltpu.VMEM((3, 3 * chans, chans), BF),
            pltpu.VMEM((3 * chans, chans), BF),
            pltpu.VMEM((3, chans, 3 * chans), BF),
            pltpu.VMEM((chans, 3 * chans), BF),
            pltpu.VMEM((f_dev + 2, rows + 2, chans, width), BF),
            pltpu.VMEM((nf, cells, c_dev), BF),
            pltpu.VMEM((nf, cells, c_dev), BF),
            pltpu.VMEM((nf, cells, c_dev), BF),
            pltpu.VMEM((cells, chans), BF),
            pltpu.VMEM((nf, cells, chans), BF),
            pltpu.VMEM((cells, chans), BF),
            pltpu.VMEM((3, group, cells, chans), BF),
            pltpu.VMEM((2, 3 * chans, (rows + 2) * width), BF),
            pltpu.VMEM(((f_dev + 2) * chans, rows * width), BF),
            pltpu.VMEM((chans, width), F32),
            pltpu.VMEM((chans, width), F32),
            dma((8,)),
            dma((10,)),
            dma((10,)),
            dma((nf,)),
            dma((nf,)),
            dma((nf,)),
            dma((nf,)),
            dma((nf,)),
            dma((nf,)),
            dma((group + 1,)),
            dma((3, group)),
        ],
        compiler_params=pltpu.CompilerParams(
            collective_id=0, has_side_effects=True, vmem_limit_bytes=56 * 1024 * 1024
        ),
        name="decoder_window",
    )(
        fine_t,
        coarse.reshape(cells, c_dev),
        jnp.swapaxes(w_qkv, 1, 2),
        w_out,
        w_up,
        gain_one,
        conv_space.reshape(3, 3 * chans, chans),
        gain_two,
        conv_time.reshape(3 * chans, chans),
    )
    return jnp.transpose(out, (0, 2, 1, 3))


def solution(mesh):
    return jax.shard_map(
        local,
        mesh=mesh,
        in_specs=(
            P("frame", None, "row", None),
            P(None, "row", "frame"),
            P(None, None, "frame"),
            P("frame", None),
            P("frame", None),
            P(),
            P(),
            P(),
            P(),
        ),
        out_specs=P("frame", None, "row", None),
        check_vma=False,
    )
```
